1024 devices in a mesh: gy: 64 (over y, x, core), gx: 16 (over z).
Axes of the slice: x: 4, y: 8, z: 16, core: 2. Of those that a mesh axis runs over, the one named last changes fastest.
Arguments:
- fields: bfloat16 [16, 1472, 2048], P(None, 'gy', 'gx'), may hold values from -6 to 6
- level_order: int32 [16], replicated, may hold values from 0 to 15, each once
- m_owner: int32 [1024], replicated, may hold values from 0 to 63, as said below
- n_count: int32 [1024], replicated, may hold values from 1 to 736, as said below
Outputs:
- spectrum: float32 [16, 1536, 2944], P('gx', 'gy')
The draws below stay inside these ranges and needn't reach their ends.
Inputs may be any that keep to these rules, and one draw needn't show every extreme that they name: `m_owner`: each owner is named by at most 24 wavenumbers m, and some owner by exactly 24. Wavenumbers n = 0 to n_count[m] - 1 are retained for m; the count for m = 0 is 736.
All inputs are finite; a program needn't handle non-finite values.
Results may differ from the reference program's by a relative error of at most 0.0066.
Values may be sent and summed in bfloat16 or wider, within the bound.
No kernel may reach another device: no remote copies, remote signals or barrier semaphores. Data moves between devices by JAX's collectives and lax.ppermute only.
A program may use at most 32 MiB of HBM per device.

```python
import math
import jax
import jax.numpy as jnp
from jax import lax

NX = 2048
NY = 1472
LEV = 16
M = 1024
NN = 736
MCAP = 24
N_GY = 64


def draw_m_owner(key, part):
    key_full = jax.random.fold_in(key, 11)
    key_rank = jax.random.fold_in(key, 12)
    key_mode = jax.random.fold_in(key, 13)
    slot_total = N_GY * MCAP
    full_owner = jax.random.randint(key_full, (), 0, N_GY)
    slot_ranks = jax.random.permutation(key_rank, slot_total).astype(jnp.int32)
    slot_owner = jnp.arange(slot_total, dtype=jnp.int32) // MCAP
    scores = slot_ranks + jnp.where(slot_owner == full_owner, 0, slot_total).astype(jnp.int32)
    ordering = jnp.argsort(scores, stable=True)
    chosen = (ordering[:M] // MCAP).astype(jnp.int32)
    mode_perm = jax.random.permutation(key_mode, M)
    return jnp.zeros((M,), jnp.int32).at[mode_perm].set(chosen)


def draw_n_count(key, part):
    key_jitter = jax.random.fold_in(key, 21)
    scaled_m = jnp.arange(M, dtype=jnp.int32)[:, None] * 1024 // M
    scaled_n = jnp.arange(NN, dtype=jnp.int32)[None, :] * 1024 // NN
    inside = (scaled_m * scaled_m + scaled_n * scaled_n <= 1024 * 1024).astype(jnp.int32)
    ellipse = jnp.sum(inside, axis=1)
    jitter = jax.random.randint(key_jitter, (M,), 0, 17)
    return jnp.minimum(NN, ellipse + jitter).astype(jnp.int32)


def steps_of(rng, shape, split, least, top_value):
    def one(dim, shards_of):
        steps = jax.random.uniform(jax.random.fold_in(jax.random.fold_in(rng, 6), dim), (shards_of,), jnp.float32, least / len(split), top_value / len(split))
        return jnp.repeat(jnp.exp(steps), shape[dim] // shards_of).reshape((-1,) + (1,) * (len(shape) - dim - 1))

    level = one(*split[0])
    for cut in split[1:]:
        level = level * one(*cut)
    return level


def centred(own_key, dims, scale, bound, split=(), held_as=jnp.bfloat16):
    drawn = scale * jax.random.normal(own_key, dims, jnp.float32)
    if split:
        drawn = drawn * steps_of(own_key, dims, split, -0.22, 0.18)
    return jnp.clip(drawn, -bound, bound).astype(held_as)


def setup_inputs(seed: int = 0) -> dict:
    key_of = jax.random.split(jax.random.key(seed), 5)
    fields = centred(key_of[0], (LEV, NY, NX), 1.0, 6.0, ((1, 64), (2, 16)))
    level_order = jax.random.permutation(key_of[1], LEV).astype(jnp.int32)
    m_owner = draw_m_owner(jax.random.fold_in(key_of[4], 71), 0)
    n_count = draw_n_count(jax.random.fold_in(key_of[4], 71), 0)
    return {"fields": fields, "level_order": level_order, "m_owner": m_owner, "n_count": n_count}


def mode_tables(extent, mode_total):
    middle = extent // 2
    points = jnp.arange(middle + 1, dtype=jnp.int32)
    orders = jnp.arange(mode_total, dtype=jnp.int32)
    phases = (points[:, None] * orders[None, :] % extent).astype(jnp.float32) * (2.0 * math.pi / extent)
    weight = jnp.where((points == 0) | (points == middle), 0.5, 1.0).astype(jnp.float32)
    factor = 1.0 / math.sqrt(extent)
    cos_even = (weight[:, None] * jnp.cos(phases) * factor).astype(jnp.bfloat16)
    sin_odd = (-jnp.sin(phases) * factor).astype(jnp.bfloat16)
    return (cos_even, sin_odd)

def fold_ends(values, along_dim):
    extent = values.shape[along_dim]
    middle = extent // 2
    leading = lax.slice_in_dim(values, 0, middle + 1, axis=along_dim)
    anchor = lax.slice_in_dim(values, 0, 1, axis=along_dim)
    trailing = jnp.flip(lax.slice_in_dim(values, middle, extent, axis=along_dim), along_dim)
    mirror = jnp.concatenate([anchor, trailing], along_dim)
    even_part = (leading.astype(jnp.float32) + mirror.astype(jnp.float32)).astype(jnp.bfloat16)
    odd_part = (leading.astype(jnp.float32) - mirror.astype(jnp.float32)).astype(jnp.bfloat16)
    return (even_part, odd_part)

def slot_table(m_owner, groups, capacity):
    mode_count = m_owner.shape[0]
    modes = jnp.arange(mode_count, dtype=jnp.int32)
    keys = (m_owner * mode_count + modes).astype(jnp.int32)
    ordering = jnp.argsort(keys, stable=True).astype(jnp.int32)
    sorted_owner = jnp.take(m_owner, ordering).astype(jnp.int32)
    owners = jnp.arange(groups, dtype=jnp.int32)
    counts = lax.optimization_barrier(jnp.sum((m_owner[:, None] == owners[None, :]).astype(jnp.int32), axis=0)).astype(jnp.int32)
    starts = (jnp.cumsum(counts) - counts).astype(jnp.int32)
    within = (modes - jnp.take(starts, sorted_owner)).astype(jnp.int32)
    slot_index = (sorted_owner * capacity + within).astype(jnp.int32)
    slot_modes = jnp.zeros((groups * capacity,), jnp.int32).at[slot_index].set(ordering)
    filled = jnp.zeros((groups * capacity,), jnp.float32).at[slot_index].set(1.0)
    return (slot_modes, filled)

def reference(fields, level_order, m_owner, n_count):
    mode_count = NX // 2
    wave_count = NY // 2
    cos_x, sin_x = mode_tables(NX, mode_count)
    cos_y, sin_y = mode_tables(NY, wave_count)
    slot_modes, filled = slot_table(m_owner, N_GY, MCAP)
    retained = (jnp.arange(wave_count, dtype=jnp.int32)[None, :] < n_count[:, None]).astype(jnp.float32)

    def one_level(level_index):
        level_grid = fields[level_index]
        even_part, odd_part = fold_ends(level_grid, 1)
        along = jnp.dot(even_part, cos_x, preferred_element_type=jnp.float32).astype(jnp.bfloat16)
        across = jnp.dot(odd_part, sin_x, preferred_element_type=jnp.float32).astype(jnp.bfloat16)
        spectra = jnp.stack([along, across], 0)
        even_y, odd_y = fold_ends(spectra, 1)
        cosine_part = jnp.einsum('cym,yn->mcn', even_y.astype(jnp.float32), cos_y.astype(jnp.float32), precision=lax.Precision.HIGHEST)
        sine_part = jnp.einsum('cym,yn->mcn', odd_y.astype(jnp.float32), sin_y.astype(jnp.float32), precision=lax.Precision.HIGHEST)
        result = jnp.stack([cosine_part, sine_part], 2) * retained[:, None, None, :]
        picked = jnp.take(result.reshape(mode_count, 4 * wave_count), slot_modes, axis=0)
        return picked * filled[:, None]
    return lax.map(one_level, level_order)
```

```python
import math

import jax
import jax.numpy as jnp
import numpy as np
from jax import lax
from jax.experimental import pallas as pl
from jax.experimental.pallas import tpu as pltpu
from jax.sharding import PartitionSpec as P

NX = 2048
NY = 1472
M = 1024
NN = 736
MCAP = 24
N_GY = 64
N_GX = 16
ROWS_Y = 23
LANE = 128
KX = M + LANE + M
F32 = jnp.float32
BF16 = jnp.bfloat16


def mode_tables(extent, mode_total):
    middle = extent // 2
    points = np.arange(middle + 1, dtype=np.int64)
    orders = np.arange(mode_total, dtype=np.int64)
    phases = (points[:, None] * orders[None, :] % extent).astype(np.float32) * np.float32(
        2.0 * math.pi / extent
    )
    weight = np.where((points == 0) | (points == middle), 0.5, 1.0).astype(np.float32)
    factor = np.float32(1.0 / math.sqrt(extent))
    cos_even = weight[:, None] * np.cos(phases) * factor
    sin_odd = -np.sin(phases) * factor
    return cos_even, sin_odd


def x_table():
    cos_x, sin_x = mode_tables(NX, M)
    table = np.zeros((M, KX), np.float32)
    table[:, : M + 1] = cos_x.T
    table[:, M + LANE :] = sin_x[:M].T
    return table.astype(BF16)


def y_tables():
    cos_y, sin_y = mode_tables(NY, NN)
    half = N_GY // 2
    cos_rows = np.zeros((half, 32, 768), np.float32)
    sin_rows = np.zeros((half, 32, 896), np.float32)
    cos_rows[:, :ROWS_Y, :NN] = cos_y[: half * ROWS_Y].reshape(half, ROWS_Y, NN)
    cos_rows[0, ROWS_Y, :NN] = cos_y[half * ROWS_Y]
    sin_rows[:, :ROWS_Y, 96 : 96 + NN] = sin_y[: half * ROWS_Y].reshape(half, ROWS_Y, NN)
    return (
        cos_rows.reshape(half * 32, 768).astype(BF16),
        sin_rows.reshape(half * 32, 896).astype(BF16),
    )


def iota(shape, dim):
    return lax.broadcasted_iota(jnp.int32, shape, dim)


def onehot(mask):
    return jnp.where(mask, 1.0, 0.0).astype(BF16)


def dot(a, b, contract_b=0):
    return lax.dot_general(a, b, (((1,), (contract_b,)), ((), ())), preferred_element_type=F32)


def order_kernel(level_ref, fields_ref, out_ref):
    for r in range(N_GX):
        out_ref[r, 0:ROWS_Y, :] = fields_ref[level_ref[0, r]]
        out_ref[r, ROWS_Y:, :] = jnp.zeros((24 - ROWS_Y, LANE), BF16)


def slot_kernel(gy_ref, owner_ref, count_ref, rows_ref, own_ref):
    blocks = M // LANE
    owner = owner_ref[...]
    hot = onehot(iota((N_GY, M), 0) == owner)
    stacked = jnp.concatenate([hot[:, b * LANE : (b + 1) * LANE] for b in range(blocks)], 0)
    source = iota((LANE, 2 * LANE), 0)
    target = iota((LANE, 2 * LANE), 1)
    prefix = dot(stacked, onehot((source < target) | (target >= LANE)))
    before = jnp.zeros((N_GY, LANE), F32)
    within = []
    for b in range(blocks):
        part = prefix[b * N_GY : (b + 1) * N_GY]
        rank = part[:, :LANE] + before
        before = before + part[:, LANE:]
        picked = hot[:, b * LANE : (b + 1) * LANE].astype(F32) * rank
        within.append(jnp.sum(picked, axis=0, keepdims=True))
    within = jnp.concatenate(within, 1).astype(jnp.int32)
    low = jnp.where(within < 16, owner * 16 + within, -1)
    high = jnp.where(within >= 16, owner * 16 + within - 16, -1)
    rows_ref[...] = jnp.concatenate([low, high], 0)
    slot = owner * MCAP + within
    mine = gy_ref[0, 0] * MCAP + iota((MCAP, M), 0) == slot
    counts = jnp.sum(jnp.where(mine, count_ref[...].astype(F32), 0.0), axis=1, keepdims=True)
    own_ref[...] = jnp.broadcast_to(counts, (MCAP, LANE)).astype(jnp.int32)


def x_kernel(grid_ref, rows_ref, table_hbm, out_ref, table_ref, sems):
    chunks = 4
    size = M // chunks
    copies = [
        pltpu.make_async_copy(
            table_hbm.at[pl.ds(i * size, size)], table_ref.at[pl.ds(i * size, size)], sems.at[i]
        )
        for i in range(chunks)
    ]
    for c in copies:
        c.start()
    k = iota((2 * LANE, LANE), 0)
    i = iota((2 * LANE, LANE), 1)
    flip = onehot(((k < LANE) & (i >= 1) & (k == LANE - i)) | ((k == LANE) & (i == 0)))
    half = N_GX // 2
    pairs = [
        jnp.concatenate([grid_ref[N_GX - 1 - b], grid_ref[(N_GX - b) % N_GX]], 1)
        for b in range(half)
    ]
    mirror = dot(jnp.concatenate(pairs, 0), flip)
    lead = [grid_ref[b].astype(F32) for b in range(half)]
    even = [(lead[b] + mirror[b * 24 : (b + 1) * 24]).astype(BF16) for b in range(half)]
    odd = [(lead[b] - mirror[b * 24 : (b + 1) * 24]).astype(BF16) for b in range(half)]
    middle = grid_ref[half].astype(F32)
    even.append((middle + middle).astype(BF16))
    even = jnp.concatenate(even, 1)
    odd = jnp.concatenate(odd, 1)
    pad = jnp.zeros((8, KX), BF16)
    top = jnp.concatenate([even, jnp.zeros((24, M), BF16)], 1)
    bottom = jnp.concatenate([jnp.zeros((24, M + LANE), BF16), odd], 1)
    folded = jnp.concatenate([top, pad, bottom, pad], 0)
    place = iota((M, M), 0)
    low = onehot(place == rows_ref[0:1, :])
    high = onehot(iota((M // 1, M), 0) == rows_ref[1:2, :])
    spectra = []
    for j in range(chunks):
        copies[j].wait()
        part = table_ref[j * size : (j + 1) * size, :]
        spectra.append(dot(part, folded, 1).astype(BF16))
    spectra = jnp.concatenate(spectra, 0)
    none = jnp.zeros((M, 64), BF16)
    first = jnp.concatenate([spectra, none], 1)
    second = jnp.concatenate([none, spectra], 1)
    placed = dot(low, first) + dot(high, second)
    out_ref[...] = placed.astype(BF16).reshape(N_GY, 16, LANE)


def y_kernel(got_ref, own_ref, cos_hbm, sin_hbm, out_ref, cos_ref, sin_ref, sems):
    copies = [
        pltpu.make_async_copy(cos_hbm, cos_ref, sems.at[0]),
        pltpu.make_async_copy(sin_hbm, sin_ref, sems.at[1]),
    ]
    for c in copies:
        c.start()
    half = N_GY // 2
    groups = half // 4
    n = iota((1, 512), 1)
    wanted_g = n // 128
    wanted_u = (n // 32) % 4
    j = n % 32
    lead_key = jnp.where(j < ROWS_Y, wanted_u * 128 + wanted_g * 32 + j, -1)
    lead_perm = onehot(iota((512, 512), 0) == lead_key)
    mirror_key = jnp.where(
        j == 0,
        (4 - wanted_u) * 128 + wanted_g * 32,
        jnp.where(j < ROWS_Y, (3 - wanted_u) * 128 + wanted_g * 32 + ROWS_Y - j, -1),
    )
    mirror_perm = onehot(iota((640, 512), 0) == mirror_key)
    middle_key = jnp.where((j == ROWS_Y) & (wanted_u == 0), wanted_g * 32, -1)
    middle_perm = onehot(iota((128, 512), 0) == middle_key)
    lead = jnp.concatenate(
        [jnp.concatenate([got_ref[4 * t + u] for u in range(4)], 1) for t in range(groups)], 0
    )
    back = jnp.concatenate(
        [
            jnp.concatenate([got_ref[(60 - 4 * t + v) % N_GY] for v in range(5)], 1)
            for t in range(groups)
        ],
        0,
    )
    lead = dot(lead, lead_perm)
    mirror = dot(back, mirror_perm)
    middle = dot(got_ref[half], middle_perm)
    even = lead + mirror
    odd = (lead - mirror).astype(BF16)
    even = jnp.concatenate([even[:16] + 2.0 * middle, even[16:]], 0).astype(BF16)

    def rows_of(v):
        return jnp.concatenate(
            [
                jnp.concatenate(
                    [v[t * 16 : (t + 1) * 16, g * LANE : (g + 1) * LANE] for t in range(groups)], 1
                )
                for g in range(4)
            ],
            0,
        )

    even = rows_of(even)
    odd = rows_of(odd)
    copies[0].wait()
    cos_part = dot(even, cos_ref[...])
    copies[1].wait()
    sin_part = dot(odd, sin_ref[...])
    both = jnp.concatenate(
        [cos_part[:, :640], cos_part[:, 640:] + sin_part[:, :LANE], sin_part[:, LANE:]], 1
    )[:, : 2 * NN]
    lane = iota((MCAP, 2 * NN), 1)
    lane = jnp.where(lane >= NN, lane - NN, lane)
    keep = lane < own_ref[:, 0:1]
    parts = []
    for c in range(2):
        part = jnp.concatenate([both[c * 16 : c * 16 + 16], both[32 + c * 16 : 40 + c * 16]], 0)
        parts.append(jnp.where(keep, part, 0.0))
    out_ref[0] = jnp.concatenate(parts, 1)


def vmem():
    return pl.BlockSpec(memory_space=pltpu.VMEM)


def smem():
    return pl.BlockSpec(memory_space=pltpu.SMEM)


def hbm():
    return pl.BlockSpec(memory_space=pl.ANY)


def order_levels(level_order, fields):
    return pl.pallas_call(
        order_kernel,
        out_shape=jax.ShapeDtypeStruct((N_GX, 24, LANE), BF16),
        in_specs=[smem(), vmem()],
        out_specs=vmem(),
        name="order_levels",
    )(level_order.reshape(1, N_GX), fields)


def find_slots(gy, m_owner, n_count):
    return pl.pallas_call(
        slot_kernel,
        out_shape=(
            jax.ShapeDtypeStruct((2, M), jnp.int32),
            jax.ShapeDtypeStruct((MCAP, LANE), jnp.int32),
        ),
        in_specs=[smem(), vmem(), vmem()],
        out_specs=(vmem(), vmem()),
        cost_estimate=pl.CostEstimate(flops=200_000_000, bytes_accessed=100_000, transcendentals=0),
        name="slots",
    )(gy.reshape(1, 1), m_owner.reshape(1, M), n_count.reshape(1, M))


def x_transform(grid, rows, table):
    return pl.pallas_call(
        x_kernel,
        out_shape=jax.ShapeDtypeStruct((N_GY, 16, LANE), BF16),
        in_specs=[vmem(), vmem(), hbm()],
        out_specs=vmem(),
        scratch_shapes=[pltpu.VMEM((M, KX), BF16), pltpu.SemaphoreType.DMA((4,))],
        name="x_transform",
    )(grid, rows, table)


def y_transform(arrived, own, cos_y, sin_y):
    return pl.pallas_call(
        y_kernel,
        out_shape=jax.ShapeDtypeStruct((1, MCAP, 4 * NN), F32),
        in_specs=[vmem(), vmem(), hbm(), hbm()],
        out_specs=vmem(),
        scratch_shapes=[
            pltpu.VMEM((1024, 768), BF16),
            pltpu.VMEM((1024, 896), BF16),
            pltpu.SemaphoreType.DMA((2,)),
        ],
        name="y_transform",
    )(arrived, own, cos_y, sin_y)


def body(fields, level_order, m_owner, n_count):
    table_x = jnp.asarray(x_table())
    cos_y, sin_y = (jnp.asarray(t) for t in y_tables())
    ordered = order_levels(level_order, fields)
    grid = lax.all_to_all(ordered, "gx", split_axis=0, concat_axis=0, tiled=True)
    rows, own = find_slots(lax.axis_index("gy"), m_owner, n_count)
    outgoing = x_transform(grid, rows, table_x)
    arrived = lax.all_to_all(outgoing, "gy", split_axis=0, concat_axis=0, tiled=True)
    return y_transform(arrived, own, cos_y, sin_y)


def solution(mesh):
    in_specs = (P(None, "gy", "gx"), P(), P(), P())
    out_specs = P("gx", "gy", None)
    return jax.shard_map(body, mesh=mesh, in_specs=in_specs, out_specs=out_specs, check_vma=False)
```

```python
import math

import jax
import jax.numpy as jnp
import numpy as np
from jax import lax
from jax.experimental import pallas as pl
from jax.experimental.pallas import tpu as pltpu
from jax.sharding import PartitionSpec as P

NX = 2048
NY = 1472
M = 1024
NN = 736
MCAP = 24
N_GY = 64
N_GX = 16
ROWS_Y = 23
LANE = 128
VMEM_LIMIT = 32 << 20
F32 = jnp.float32
BF16 = jnp.bfloat16


def mode_tables(extent, mode_total):
    middle = extent // 2
    points = np.arange(middle + 1, dtype=np.int64)
    orders = np.arange(mode_total, dtype=np.int64)
    phases = (points[:, None] * orders[None, :] % extent).astype(np.float32) * np.float32(
        2.0 * math.pi / extent
    )
    weight = np.where((points == 0) | (points == middle), 0.5, 1.0).astype(np.float32)
    factor = np.float32(1.0 / math.sqrt(extent))
    cos_even = weight[:, None] * np.cos(phases) * factor
    sin_odd = -np.sin(phases) * factor
    return cos_even, sin_odd


def x_tables():
    cos_x, sin_x = mode_tables(NX, M)
    cos_rows = np.zeros((M + LANE, M), np.float32)
    cos_rows[: M + 1] = cos_x
    return cos_rows.astype(BF16), sin_x[:M].astype(BF16)


def y_tables():
    cos_y, sin_y = mode_tables(NY, NN)
    half = N_GY // 2
    cos_rows = np.zeros((half, 32, 768), np.float32)
    sin_rows = np.zeros((half, 32, 896), np.float32)
    cos_rows[:, :ROWS_Y, :NN] = cos_y[: half * ROWS_Y].reshape(half, ROWS_Y, NN)
    cos_rows[0, ROWS_Y, :NN] = cos_y[half * ROWS_Y]
    sin_rows[:, :ROWS_Y, 96 : 96 + NN] = sin_y[: half * ROWS_Y].reshape(half, ROWS_Y, NN)
    return (
        cos_rows.reshape(half * 32, 768).astype(BF16),
        sin_rows.reshape(half * 32, 896).astype(BF16),
    )


def iota(shape, dim):
    return lax.broadcasted_iota(jnp.int32, shape, dim)


def onehot(mask):
    return jnp.where(mask, 1.0, 0.0).astype(BF16)


def dot(a, b, contract_b=0):
    return lax.dot_general(a, b, (((1,), (contract_b,)), ((), ())), preferred_element_type=F32)


def order_kernel(
    level_hbm, fields_hbm, owner_hbm, count_hbm, out_ref, rows_ref, own_ref,
    level_ref, fields_ref, owner_ref, count_ref, sems,
):
    fetches = [
        pltpu.make_async_copy(source, target, sems.at[i])
        for i, (source, target) in enumerate(
            (
                (level_hbm, level_ref),
                (fields_hbm, fields_ref),
                (owner_hbm, owner_ref),
                (count_hbm, count_ref),
            )
        )
    ]
    for fetch in fetches:
        fetch.start()
    fetches[0].wait()
    rows = N_GX * 24
    row = iota((rows, 1), 0)
    level = jnp.zeros((rows, 1), jnp.int32)
    for r in range(N_GX):
        level = jnp.where(row >= r * 24, level_ref[0, r], level)
    y = row % 24
    key = jnp.where(y < ROWS_Y, y * N_GX + level, -1)
    pick = onehot(iota((rows, 24 * N_GX), 1) == key)
    for fetch in fetches[1:]:
        fetch.wait()
    data = fields_ref[...].reshape(ROWS_Y * N_GX, LANE)
    data = jnp.concatenate([data, jnp.zeros((N_GX, LANE), BF16)], 0)
    out_ref[...] = dot(pick, data).astype(BF16).reshape(N_GX, 24, LANE)
    find_slots(owner_ref[...], count_ref[...], rows_ref, own_ref)


def find_slots(owner, count, rows_ref, own_ref):
    blocks = M // LANE
    hot = onehot(iota((N_GY, M), 0) == owner)
    stacked = jnp.concatenate([hot[:, b * LANE : (b + 1) * LANE] for b in range(blocks)], 0)
    source = iota((LANE, 2 * LANE), 0)
    target = iota((LANE, 2 * LANE), 1)
    prefix = dot(stacked, onehot((source < target) | (target >= LANE)))
    before = jnp.zeros((N_GY, LANE), F32)
    within = []
    for b in range(blocks):
        part = prefix[b * N_GY : (b + 1) * N_GY]
        rank = part[:, :LANE] + before
        before = before + part[:, LANE:]
        picked = hot[:, b * LANE : (b + 1) * LANE].astype(F32) * rank
        within.append(jnp.sum(picked, axis=0, keepdims=True))
    within = jnp.concatenate(within, 1).astype(jnp.int32)
    low = jnp.where(within < 16, owner * 16 + within, -1)
    high = jnp.where(within >= 16, owner * 8 + within - 16, -1)
    rows_ref[...] = jnp.concatenate([low, high], 0)
    mine = lax.axis_index("gy") * MCAP + iota((MCAP, M), 0) == owner * MCAP + within
    counts = jnp.sum(jnp.where(mine, count.astype(F32), 0.0), axis=1, keepdims=True)
    own_ref[...] = jnp.broadcast_to(counts, (MCAP, LANE)).astype(jnp.int32)


def x_kernel(grid_ref, rows_ref, cos_ref, sin_ref, out_ref):
    low = onehot(iota((N_GY * 16, M), 0) == rows_ref[0:1, :])
    high = onehot(iota((N_GY * 8, M), 0) == rows_ref[1:2, :])
    k = iota((2 * LANE, LANE), 0)
    i = iota((2 * LANE, LANE), 1)
    flip = onehot(((k < LANE) & (i >= 1) & (k == LANE - i)) | ((k == LANE) & (i == 0)))
    half = N_GX // 2
    pairs = [
        jnp.concatenate([grid_ref[N_GX - 1 - b], grid_ref[(N_GX - b) % N_GX]], 1)
        for b in range(half)
    ]
    mirror = dot(jnp.concatenate(pairs, 0), flip)
    lead = [grid_ref[b].astype(F32) for b in range(half)]
    even = [(lead[b] + mirror[b * 24 : (b + 1) * 24]).astype(BF16) for b in range(half)]
    odd = [(lead[b] - mirror[b * 24 : (b + 1) * 24]).astype(BF16) for b in range(half)]
    middle = grid_ref[half].astype(F32)
    even.append((middle + middle).astype(BF16))
    across = dot(jnp.concatenate(odd, 1), sin_ref[...])
    along = dot(jnp.concatenate(even, 1), cos_ref[...])
    pad = jnp.zeros((8, M), F32)
    spectra = jnp.concatenate([along, pad, across, pad], 0).astype(BF16)
    none = jnp.zeros((64, M), BF16)
    low = dot(low, jnp.concatenate([spectra, none], 0), 1).reshape(N_GY, 16, LANE)
    high = dot(high, jnp.concatenate([none, spectra], 0), 1).reshape(N_GY, 8, LANE)
    out_ref[:, :8, :] = (low[:, :8] + high).astype(BF16)
    out_ref[:, 8:, :] = low[:, 8:].astype(BF16)


def y_kernel(got_ref, own_ref, cos_ref, sin_ref, out_ref):
    half = N_GY // 2
    groups = half // 4
    n = iota((1, 512), 1)
    wanted_g = n // 128
    wanted_u = (n // 32) % 4
    j = n % 32
    lead_key = jnp.where(j < ROWS_Y, wanted_u * 128 + wanted_g * 32 + j, -1)
    lead_perm = onehot(iota((512, 512), 0) == lead_key)
    mirror_key = jnp.where(
        j == 0,
        (4 - wanted_u) * 128 + wanted_g * 32,
        jnp.where(j < ROWS_Y, (3 - wanted_u) * 128 + wanted_g * 32 + ROWS_Y - j, -1),
    )
    mirror_perm = onehot(iota((640, 512), 0) == mirror_key)
    middle_key = jnp.where((j == ROWS_Y) & (wanted_u == 0), wanted_g * 32, -1)
    middle_perm = onehot(iota((128, 512), 0) == middle_key)
    lead = jnp.concatenate(
        [jnp.concatenate([got_ref[4 * t + u] for u in range(4)], 1) for t in range(groups)], 0
    )
    back = jnp.concatenate(
        [
            jnp.concatenate([got_ref[(60 - 4 * t + v) % N_GY] for v in range(5)], 1)
            for t in range(groups)
        ],
        0,
    )
    lead = dot(lead, lead_perm)
    mirror = dot(back, mirror_perm)
    middle = dot(got_ref[half], middle_perm)
    even = lead + mirror
    odd = (lead - mirror).astype(BF16)
    even = jnp.concatenate([even[:16] + 2.0 * middle, even[16:]], 0).astype(BF16)

    def rows_of(v):
        return jnp.concatenate(
            [
                jnp.concatenate(
                    [v[t * 16 : (t + 1) * 16, g * LANE : (g + 1) * LANE] for t in range(groups)], 1
                )
                for g in range(4)
            ],
            0,
        )

    even = rows_of(even)
    odd = rows_of(odd)
    sin_part = dot(odd, sin_ref[...])
    cos_part = dot(even, cos_ref[...])
    both = jnp.concatenate(
        [cos_part[:, :640], cos_part[:, 640:] + sin_part[:, :LANE], sin_part[:, LANE:]], 1
    )[:, : 2 * NN]
    lane = iota((MCAP, 2 * NN), 1)
    lane = jnp.where(lane >= NN, lane - NN, lane)
    keep = lane < own_ref[:, 0:1]
    parts = []
    for c in range(2):
        part = jnp.concatenate([both[c * 16 : c * 16 + 16], both[32 + c * 16 : 40 + c * 16]], 0)
        parts.append(jnp.where(keep, part, 0.0))
    out_ref[0] = jnp.concatenate(parts, 1)


def vmem():
    return pl.BlockSpec(memory_space=pltpu.VMEM)


def hbm():
    return pl.BlockSpec(memory_space=pltpu.HBM)


def held(x):
    return pltpu.with_memory_space_constraint(x, pltpu.VMEM)


def far(x):
    return pltpu.with_memory_space_constraint(x, pltpu.HBM)


def order_levels(level_order, fields, m_owner, n_count):
    args = (
        level_order.reshape(1, N_GX),
        fields.transpose(1, 0, 2),
        m_owner.reshape(1, M),
        n_count.reshape(1, M),
    )
    return pl.pallas_call(
        order_kernel,
        out_shape=(
            pltpu.VMEM((N_GX, 24, LANE), BF16),
            pltpu.VMEM((2, M), jnp.int32),
            pltpu.VMEM((MCAP, LANE), jnp.int32),
        ),
        in_specs=[hbm()] * 4,
        out_specs=(vmem(),) * 3,
        scratch_shapes=[
            pltpu.SMEM((1, N_GX), jnp.int32),
            pltpu.VMEM(args[1].shape, BF16),
            pltpu.VMEM((1, M), jnp.int32),
            pltpu.VMEM((1, M), jnp.int32),
            pltpu.SemaphoreType.DMA((4,)),
        ],
        name="order_levels",
        cost_estimate=pl.CostEstimate(flops=4000000000, bytes_accessed=100000, transcendentals=0),
        compiler_params=pltpu.CompilerParams(vmem_limit_bytes=VMEM_LIMIT),
    )(*(far(x) for x in args))


def x_transform(grid, rows, cos_x, sin_x):
    return pl.pallas_call(
        x_kernel,
        out_shape=pltpu.VMEM((N_GY, 16, LANE), BF16),
        in_specs=[vmem(), vmem(), vmem(), vmem()],
        out_specs=vmem(),
        name="x_transform",
        compiler_params=pltpu.CompilerParams(vmem_limit_bytes=VMEM_LIMIT),
    )(held(grid), held(rows), held(cos_x), held(sin_x))


def y_transform(arrived, own, cos_y, sin_y):
    return pl.pallas_call(
        y_kernel,
        out_shape=jax.ShapeDtypeStruct((1, MCAP, 4 * NN), F32),
        in_specs=[vmem(), vmem(), vmem(), vmem()],
        out_specs=vmem(),
        name="y_transform",
        compiler_params=pltpu.CompilerParams(vmem_limit_bytes=VMEM_LIMIT),
    )(held(arrived), held(own), held(cos_y), held(sin_y))


def body(fields, level_order, m_owner, n_count):
    cos_x, sin_x = (jnp.asarray(t) for t in x_tables())
    cos_y, sin_y = (jnp.asarray(t) for t in y_tables())
    ordered, rows, own = order_levels(level_order, fields, m_owner, n_count)
    grid = lax.all_to_all(ordered, "gx", split_axis=0, concat_axis=0, tiled=True)
    outgoing = x_transform(grid, rows, cos_x, sin_x)
    arrived = lax.all_to_all(outgoing, "gy", split_axis=0, concat_axis=0, tiled=True)
    return y_transform(arrived, own, cos_y, sin_y)


def solution(mesh):
    in_specs = (P(None, "gy", "gx"), P(), P(), P())
    out_specs = P("gx", "gy", None)
    return jax.shard_map(body, mesh=mesh, in_specs=in_specs, out_specs=out_specs, check_vma=False)
```

```python
import math

import jax
import jax.numpy as jnp
import numpy as np
from jax import lax
from jax.experimental import pallas as pl
from jax.experimental.pallas import tpu as pltpu
from jax.sharding import PartitionSpec as P

NX = 2048
NY = 1472
M = 1024
NN = 736
MCAP = 24
HALF = MCAP // 2
N_GY = 64
N_GX = 16
ROWS_Y = 23
LANE = 128
VMEM_LIMIT = 32 << 20
F32 = jnp.float32
BF16 = jnp.bfloat16


def mode_tables(extent, mode_total):
    middle = extent // 2
    points = np.arange(middle + 1, dtype=np.int64)
    orders = np.arange(mode_total, dtype=np.int64)
    phases = (points[:, None] * orders[None, :] % extent).astype(np.float32) * np.float32(
        2.0 * math.pi / extent
    )
    weight = np.where((points == 0) | (points == middle), 0.5, 1.0).astype(np.float32)
    factor = np.float32(1.0 / math.sqrt(extent))
    cos_even = weight[:, None] * np.cos(phases) * factor
    sin_odd = -np.sin(phases) * factor
    return cos_even, sin_odd


def x_tables():
    cos_x, sin_x = mode_tables(NX, M)
    cos_rows = np.zeros((M + LANE, M), np.float32)
    cos_rows[: M + 1] = cos_x
    return cos_rows.astype(BF16), sin_x[:M].astype(BF16)


def y_tables():
    cos_y, sin_y = mode_tables(NY, NN)
    half = N_GY // 2
    cos_rows = np.zeros((half, 32, 768), np.float32)
    sin_rows = np.zeros((half, 32, 896), np.float32)
    cos_rows[:, :ROWS_Y, :NN] = cos_y[: half * ROWS_Y].reshape(half, ROWS_Y, NN)
    cos_rows[0, ROWS_Y, :NN] = cos_y[half * ROWS_Y]
    sin_rows[:, :ROWS_Y, 96 : 96 + NN] = sin_y[: half * ROWS_Y].reshape(half, ROWS_Y, NN)
    return (
        cos_rows.reshape(half * 32, 768).astype(BF16),
        sin_rows.reshape(half * 32, 896).astype(BF16),
    )


def x_flip():
    flip = np.zeros((2 * LANE, LANE), np.float32)
    for i in range(1, LANE):
        flip[LANE - i, i] = 1.0
    flip[LANE, 0] = 1.0
    return flip.astype(BF16)


def y_selections():
    lead = np.zeros((4 * LANE, 4 * LANE), np.float32)
    mirror = np.zeros((5 * LANE, 4 * LANE), np.float32)
    middle = np.zeros((LANE, 4 * LANE), np.float32)
    for g in range(4):
        middle[32 * g, LANE * g + ROWS_Y] = 1.0
        for u in range(4):
            for j in range(ROWS_Y):
                n = LANE * g + 32 * u + j
                lead[LANE * u + 32 * g + j, n] = 1.0
                if j:
                    mirror[LANE * (3 - u) + 32 * g + ROWS_Y - j, n] = 1.0
                else:
                    mirror[LANE * (4 - u) + 32 * g, n] = 1.0
    return lead.astype(BF16), mirror.astype(BF16), middle.astype(BF16)


def iota(shape, dim):
    return lax.broadcasted_iota(jnp.int32, shape, dim)


def onehot(mask):
    return jnp.where(mask, 1.0, 0.0).astype(BF16)


def dot(a, b, contract_b=0):
    return lax.dot_general(a, b, (((1,), (contract_b,)), ((), ())), preferred_element_type=F32)


def order_kernel(
    level_hbm, fields_hbm, owner_hbm, count_hbm, out_ref, rows_ref, own_ref,
    level_ref, fields_ref, owner_ref, count_ref, sems,
):
    fetches = [
        pltpu.make_async_copy(source, target, sems.at[i])
        for i, (source, target) in enumerate(
            (
                (level_hbm, level_ref),
                (fields_hbm, fields_ref),
                (owner_hbm, owner_ref),
                (count_hbm, count_ref),
            )
        )
    ]
    for fetch in fetches:
        fetch.start()
    source = iota((LANE, 2 * LANE), 0)
    target = iota((LANE, 2 * LANE), 1)
    earlier = onehot((source < target) | (target >= LANE))
    fetches[0].wait()
    rows = N_GX * 24
    lane = iota((24, rows), 1)
    y = iota((24, rows), 0)
    lane = jnp.where(y < ROWS_Y, lane - y * N_GX, -1)
    pick = [jnp.where(lane == level_ref[0, r], 1.0, 0.0) for r in range(N_GX)]
    pick = jnp.concatenate(pick, 0).astype(BF16)
    for fetch in fetches[1:]:
        fetch.wait()
    data = fields_ref[...].reshape(ROWS_Y * N_GX, LANE)
    data = jnp.concatenate([data, jnp.zeros((N_GX, LANE), BF16)], 0)
    out_ref[...] = dot(pick, data).astype(BF16).reshape(N_GX, 24, LANE)
    find_slots(owner_ref[...], count_ref[...], earlier, rows_ref, own_ref)


def find_slots(owner, count, earlier, rows_ref, own_ref):
    blocks = M // LANE
    hot = onehot(iota((N_GY, M), 0) == owner)
    stacked = jnp.concatenate([hot[:, b * LANE : (b + 1) * LANE] for b in range(blocks)], 0)
    prefix = dot(stacked, earlier)
    before = jnp.zeros((N_GY, LANE), F32)
    within = []
    for b in range(blocks):
        part = prefix[b * N_GY : (b + 1) * N_GY]
        rank = part[:, :LANE] + before
        before = before + part[:, LANE:]
        picked = hot[:, b * LANE : (b + 1) * LANE].astype(F32) * rank
        within.append(jnp.sum(picked, axis=0, keepdims=True))
    within = jnp.concatenate(within, 1).astype(jnp.int32)
    low = jnp.where(within < HALF, owner * HALF + within, -1)
    high = jnp.where(within >= HALF, owner * HALF + within - HALF, -1)
    rows_ref[...] = jnp.concatenate([low, high], 0)
    mine = lax.axis_index("gy") * MCAP + iota((MCAP, M), 0) == owner * MCAP + within
    counts = jnp.sum(jnp.where(mine, count.astype(F32), 0.0), axis=1, keepdims=True)
    own_ref[...] = jnp.broadcast_to(counts, (MCAP, LANE)).astype(jnp.int32)


def slot_rows(keys):
    row = iota((256, LANE), 0).astype(F32).astype(BF16)
    row = jnp.concatenate([row] * (M // LANE), 1)
    blocks = []
    for b in range(N_GY * HALF // 256):
        key = keys - 256 * b
        key = jnp.where((key >= 0) & (key < 256), key, -1).astype(F32).astype(BF16)
        blocks.append(jnp.where(row == key, jnp.ones((), BF16), jnp.zeros((), BF16)))
    return jnp.concatenate(blocks, 0)


def x_kernel(grid_ref, rows_ref, cos_ref, sin_ref, flip_ref, out_ref):
    low = slot_rows(rows_ref[0:1, :])
    high = slot_rows(rows_ref[1:2, :])
    half = N_GX // 2
    pairs = [
        jnp.concatenate([grid_ref[N_GX - 1 - b], grid_ref[(N_GX - b) % N_GX]], 1)
        for b in range(half)
    ]
    mirror = dot(jnp.concatenate(pairs, 0), flip_ref[...])
    lead = [grid_ref[b].astype(F32) for b in range(half)]
    even = [(lead[b] + mirror[b * 24 : (b + 1) * 24]).astype(BF16) for b in range(half)]
    odd = [(lead[b] - mirror[b * 24 : (b + 1) * 24]).astype(BF16) for b in range(half)]
    middle = grid_ref[half].astype(F32)
    even.append((middle + middle).astype(BF16))
    across = dot(jnp.concatenate(odd, 1), sin_ref[...])
    along = dot(jnp.concatenate(even, 1), cos_ref[...])
    pad = jnp.zeros((8, M), F32)
    spectra = jnp.concatenate([along, pad, across, pad], 0).astype(BF16)
    none = jnp.zeros((64, M), BF16)
    placed = dot(low, jnp.concatenate([spectra, none], 0), 1)
    placed = placed + dot(high, jnp.concatenate([none, spectra], 0), 1)
    out_ref[...] = placed.astype(BF16)


def y_kernel(
    got_ref, own_ref, cos_ref, sin_ref, lead_ref, mirror_ref, middle_ref, out_ref, wide_ref
):
    half = N_GY // 2
    groups = half // 4
    wide_ref[: N_GY * HALF, :] = got_ref[...]
    wide_ref[N_GY * HALF :, :] = jnp.zeros((16, LANE), BF16)
    got = [wide_ref[HALF * s : HALF * s + 16, :] for s in range(N_GY)]
    lead = jnp.concatenate(
        [jnp.concatenate([got[4 * t + u] for u in range(4)], 1) for t in range(groups)], 0
    )
    back = jnp.concatenate(
        [
            jnp.concatenate([got[(60 - 4 * t + v) % N_GY] for v in range(5)], 1)
            for t in range(groups)
        ],
        0,
    )
    lead = dot(lead, lead_ref[...])
    mirror = dot(back, mirror_ref[...])
    middle = dot(got[half], middle_ref[...])
    even = lead + mirror
    odd = (lead - mirror).astype(BF16)
    even = jnp.concatenate([even[:16] + 2.0 * middle, even[16:]], 0).astype(BF16)

    def rows_of(v):
        return jnp.concatenate(
            [
                jnp.concatenate(
                    [v[t * 16 : (t + 1) * 16, g * LANE : (g + 1) * LANE] for t in range(groups)], 1
                )
                for g in range(4)
            ],
            0,
        )

    even = rows_of(even)
    odd = rows_of(odd)
    sin_part = dot(odd, sin_ref[...])
    cos_part = dot(even, cos_ref[...])
    both = jnp.concatenate(
        [cos_part[:, :640], cos_part[:, 640:] + sin_part[:, :LANE], sin_part[:, LANE:]], 1
    )[:, : 2 * NN]
    lane = iota((MCAP, 2 * NN), 1)
    lane = jnp.where(lane >= NN, lane - NN, lane)
    keep = lane < own_ref[:, 0:1]
    parts = []
    for c in range(2):
        part = jnp.concatenate(
            [both[c * 16 : c * 16 + HALF], both[32 + c * 16 : 32 + c * 16 + HALF]], 0
        )
        parts.append(jnp.where(keep, part, 0.0))
    out_ref[0] = jnp.concatenate(parts, 1)


def vmem():
    return pl.BlockSpec(memory_space=pltpu.VMEM)


def hbm():
    return pl.BlockSpec(memory_space=pltpu.HBM)


def held(x):
    return pltpu.with_memory_space_constraint(x, pltpu.VMEM)


def far(x):
    return pltpu.with_memory_space_constraint(x, pltpu.HBM)


def order_levels(level_order, fields, m_owner, n_count):
    args = (
        level_order.reshape(1, N_GX),
        fields.transpose(1, 0, 2),
        m_owner.reshape(1, M),
        n_count.reshape(1, M),
    )
    return pl.pallas_call(
        order_kernel,
        out_shape=(
            pltpu.VMEM((N_GX, 24, LANE), BF16),
            pltpu.VMEM((2, M), jnp.int32),
            pltpu.VMEM((MCAP, LANE), jnp.int32),
        ),
        in_specs=[hbm()] * 4,
        out_specs=(vmem(),) * 3,
        scratch_shapes=[
            pltpu.SMEM((1, N_GX), jnp.int32),
            pltpu.VMEM(args[1].shape, BF16),
            pltpu.VMEM((1, M), jnp.int32),
            pltpu.VMEM((1, M), jnp.int32),
            pltpu.SemaphoreType.DMA((4,)),
        ],
        name="order_levels",
        cost_estimate=pl.CostEstimate(flops=4000000000, bytes_accessed=100000, transcendentals=0),
        compiler_params=pltpu.CompilerParams(vmem_limit_bytes=VMEM_LIMIT),
    )(*(far(x) for x in args))


def x_transform(grid, rows, cos_x, sin_x):
    args = (grid, rows, cos_x, sin_x, jnp.asarray(x_flip()))
    return pl.pallas_call(
        x_kernel,
        out_shape=pltpu.VMEM((N_GY * HALF, LANE), BF16),
        in_specs=[vmem() for _ in args],
        out_specs=vmem(),
        name="x_transform",
        compiler_params=pltpu.CompilerParams(vmem_limit_bytes=VMEM_LIMIT),
    )(*(held(x) for x in args))


def y_transform(arrived, own, cos_y, sin_y):
    args = (arrived, own, cos_y, sin_y, *(jnp.asarray(t) for t in y_selections()))
    return pl.pallas_call(
        y_kernel,
        out_shape=jax.ShapeDtypeStruct((1, MCAP, 4 * NN), F32),
        in_specs=[vmem() for _ in args],
        out_specs=vmem(),
        scratch_shapes=[pltpu.VMEM((N_GY * HALF + 16, LANE), BF16)],
        name="y_transform",
        compiler_params=pltpu.CompilerParams(vmem_limit_bytes=VMEM_LIMIT),
    )(*(held(x) for x in args))


def body(fields, level_order, m_owner, n_count):
    cos_x, sin_x = (jnp.asarray(t) for t in x_tables())
    cos_y, sin_y = (jnp.asarray(t) for t in y_tables())
    ordered, rows, own = order_levels(level_order, fields, m_owner, n_count)
    grid = lax.all_to_all(ordered, "gx", split_axis=0, concat_axis=0, tiled=True)
    outgoing = x_transform(grid, rows, cos_x, sin_x)
    outgoing = outgoing.reshape(N_GY * HALF // 4, 4, LANE)
    arrived = lax.all_to_all(outgoing, "gy", split_axis=0, concat_axis=0, tiled=True)
    arrived = arrived.reshape(N_GY * HALF, LANE)
    return y_transform(arrived, own, cos_y, sin_y)


def solution(mesh):
    in_specs = (P(None, "gy", "gx"), P(), P(), P())
    out_specs = P("gx", "gy", None)
    return jax.shard_map(body, mesh=mesh, in_specs=in_specs, out_specs=out_specs, check_vma=False)
```

```python
import math

import jax
import jax.numpy as jnp
import numpy as np
from jax import lax
from jax.experimental import pallas as pl
from jax.experimental.pallas import tpu as pltpu
from jax.sharding import PartitionSpec as P

NX = 2048
NY = 1472
M = 1024
NN = 736
MCAP = 24
HALF = MCAP // 2
N_GY = 64
N_GX = 16
ROWS_Y = 23
FETCH_ROWS = 4
LANE = 128
VMEM_LIMIT = 32 << 20
F32 = jnp.float32
BF16 = jnp.bfloat16


def mode_tables(extent, mode_total):
    middle = extent // 2
    points = np.arange(middle + 1, dtype=np.int64)
    orders = np.arange(mode_total, dtype=np.int64)
    phases = (points[:, None] * orders[None, :] % extent).astype(np.float32) * np.float32(
        2.0 * math.pi / extent
    )
    weight = np.where((points == 0) | (points == middle), 0.5, 1.0).astype(np.float32)
    factor = np.float32(1.0 / math.sqrt(extent))
    cos_even = weight[:, None] * np.cos(phases) * factor
    sin_odd = -np.sin(phases) * factor
    return cos_even, sin_odd


def x_tables():
    cos_x, sin_x = mode_tables(NX, M)
    cos_rows = np.zeros((M + LANE, M), np.float32)
    cos_rows[: M + 1] = cos_x
    return cos_rows.astype(BF16), sin_x[:M].astype(BF16)


def y_tables():
    cos_y, sin_y = mode_tables(NY, NN)
    half = N_GY // 2
    cos_rows = np.zeros((half, 32, 768), np.float32)
    sin_rows = np.zeros((half, 32, 896), np.float32)
    cos_rows[:, :ROWS_Y, :NN] = cos_y[: half * ROWS_Y].reshape(half, ROWS_Y, NN)
    cos_rows[0, ROWS_Y, :NN] = cos_y[half * ROWS_Y]
    sin_rows[:, :ROWS_Y, 96 : 96 + NN] = sin_y[: half * ROWS_Y].reshape(half, ROWS_Y, NN)
    return (
        cos_rows.reshape(half * 32, 768).astype(BF16),
        sin_rows.reshape(half * 32, 896).astype(BF16),
    )


def x_flip():
    flip = np.zeros((2 * LANE, LANE), np.float32)
    for i in range(1, LANE):
        flip[LANE - i, i] = 1.0
    flip[LANE, 0] = 1.0
    return flip.astype(BF16)


def y_selections():
    lead = np.zeros((4 * LANE, 4 * LANE), np.float32)
    mirror = np.zeros((5 * LANE, 4 * LANE), np.float32)
    middle = np.zeros((LANE, 4 * LANE), np.float32)
    for g in range(4):
        middle[32 * g, LANE * g + ROWS_Y] = 1.0
        for u in range(4):
            for j in range(ROWS_Y):
                n = LANE * g + 32 * u + j
                lead[LANE * u + 32 * g + j, n] = 1.0
                if j:
                    mirror[LANE * (3 - u) + 32 * g + ROWS_Y - j, n] = 1.0
                else:
                    mirror[LANE * (4 - u) + 32 * g, n] = 1.0
    return lead.astype(BF16), mirror.astype(BF16), middle.astype(BF16)


def iota(shape, dim):
    return lax.broadcasted_iota(jnp.int32, shape, dim)


def onehot(mask):
    return jnp.where(mask, 1.0, 0.0).astype(BF16)


def dot(a, b, contract_b=0):
    return lax.dot_general(a, b, (((1,), (contract_b,)), ((), ())), preferred_element_type=F32)


def order_kernel(level_hbm, fields_hbm, out_ref, level_ref, fields_ref, sems):
    fetches = [pltpu.make_async_copy(level_hbm, level_ref, sems.at[0])]
    for i, first in enumerate(range(0, ROWS_Y, FETCH_ROWS)):
        part = pl.ds(first, min(FETCH_ROWS, ROWS_Y - first))
        fetches.append(
            pltpu.make_async_copy(fields_hbm.at[part], fields_ref.at[part], sems.at[i + 1])
        )
    for fetch in fetches:
        fetch.start()
    rows = N_GX * 24
    lane = iota((24, rows), 1)
    y = iota((24, rows), 0)
    lane = jnp.where(y < ROWS_Y, lane - y * N_GX, -1)
    fetches[0].wait()
    pick = [jnp.where(lane == level_ref[0, r], 1.0, 0.0) for r in range(N_GX)]
    pick = jnp.concatenate(pick, 0).astype(BF16)
    for fetch in fetches[1:]:
        fetch.wait()
    data = fields_ref[...].reshape(ROWS_Y * N_GX, LANE)
    data = jnp.concatenate([data, jnp.zeros((N_GX, LANE), BF16)], 0)
    out_ref[...] = dot(pick, data).astype(BF16).reshape(N_GX, 24, LANE)


def find_slots(owner, count, own_ref):
    blocks = M // LANE
    hot = onehot(iota((N_GY, M), 0) == owner)
    stacked = jnp.concatenate([hot[:, b * LANE : (b + 1) * LANE] for b in range(blocks)], 0)
    source = iota((LANE, 2 * LANE), 0)
    target = iota((LANE, 2 * LANE), 1)
    prefix = dot(stacked, onehot((source < target) | (target >= LANE)))
    before = jnp.zeros((N_GY, LANE), F32)
    within = []
    for b in range(blocks):
        part = prefix[b * N_GY : (b + 1) * N_GY]
        rank = part[:, :LANE] + before
        before = before + part[:, LANE:]
        picked = hot[:, b * LANE : (b + 1) * LANE].astype(F32) * rank
        within.append(jnp.sum(picked, axis=0, keepdims=True))
    within = jnp.concatenate(within, 1).astype(jnp.int32)
    low = jnp.where(within < HALF, owner * HALF + within, -1)
    high = jnp.where(within >= HALF, owner * HALF + within - HALF, -1)
    mine = lax.axis_index("gy") * MCAP + iota((MCAP, M), 0) == owner * MCAP + within
    counts = jnp.sum(jnp.where(mine, count.astype(F32), 0.0), axis=1, keepdims=True)
    own_ref[...] = jnp.broadcast_to(counts, (MCAP, LANE)).astype(jnp.int32)
    return low, high


def slot_rows(keys):
    row = iota((256, LANE), 0).astype(F32).astype(BF16)
    row = jnp.concatenate([row] * (M // LANE), 1)
    blocks = []
    for b in range(N_GY * HALF // 256):
        key = keys - 256 * b
        key = jnp.where((key >= 0) & (key < 256), key, -1).astype(F32).astype(BF16)
        blocks.append(jnp.where(row == key, jnp.ones((), BF16), jnp.zeros((), BF16)))
    return jnp.concatenate(blocks, 0)


def x_kernel(grid_ref, owner_ref, count_ref, cos_ref, sin_ref, flip_ref, out_ref, own_ref):
    keys = find_slots(owner_ref[...], count_ref[...], own_ref)
    half = N_GX // 2
    pairs = [
        jnp.concatenate([grid_ref[N_GX - 1 - b], grid_ref[(N_GX - b) % N_GX]], 1)
        for b in range(half)
    ]
    mirror = dot(jnp.concatenate(pairs, 0), flip_ref[...])
    lead = [grid_ref[b].astype(F32) for b in range(half)]
    even = [(lead[b] + mirror[b * 24 : (b + 1) * 24]).astype(BF16) for b in range(half)]
    odd = [(lead[b] - mirror[b * 24 : (b + 1) * 24]).astype(BF16) for b in range(half)]
    middle = grid_ref[half].astype(F32)
    even.append((middle + middle).astype(BF16))
    across = dot(jnp.concatenate(odd, 1), sin_ref[...])
    along = dot(jnp.concatenate(even, 1), cos_ref[...])
    pad = jnp.zeros((8, M), F32)
    spectra = jnp.concatenate([along, pad, across, pad], 0).astype(BF16)
    none = jnp.zeros((64, M), BF16)
    low, high = (slot_rows(k) for k in keys)
    placed = dot(low, jnp.concatenate([spectra, none], 0), 1)
    placed = placed + dot(high, jnp.concatenate([none, spectra], 0), 1)
    out_ref[...] = placed.astype(BF16)


def y_kernel(
    got_ref, own_ref, cos_ref, sin_ref, lead_ref, mirror_ref, middle_ref, out_hbm, wide_ref, out_ref, sems
):
    half = N_GY // 2
    groups = half // 4
    wide_ref[: N_GY * HALF, :] = got_ref[...]
    wide_ref[N_GY * HALF :, :] = jnp.zeros((16, LANE), BF16)
    got = [wide_ref[HALF * s : HALF * s + 16, :] for s in range(N_GY)]
    lead = jnp.concatenate(
        [jnp.concatenate([got[4 * t + u] for u in range(4)], 1) for t in range(groups)], 0
    )
    back = jnp.concatenate(
        [
            jnp.concatenate([got[(60 - 4 * t + v) % N_GY] for v in range(5)], 1)
            for t in range(groups)
        ],
        0,
    )
    lead = dot(lead, lead_ref[...])
    mirror = dot(back, mirror_ref[...])
    middle = dot(got[half], middle_ref[...])
    even = lead + mirror
    odd = (lead - mirror).astype(BF16)
    even = jnp.concatenate([even[:16] + 2.0 * middle, even[16:]], 0).astype(BF16)

    def rows_of(v):
        return jnp.concatenate(
            [
                jnp.concatenate(
                    [v[t * 16 : (t + 1) * 16, g * LANE : (g + 1) * LANE] for t in range(groups)], 1
                )
                for g in range(4)
            ],
            0,
        )

    even = rows_of(even)
    odd = rows_of(odd)
    sin_part = dot(odd, sin_ref[...])
    cos_part = dot(even, cos_ref[...])
    both = jnp.concatenate(
        [cos_part[:, :640], cos_part[:, 640:] + sin_part[:, :LANE], sin_part[:, LANE:]], 1
    )[:, : 2 * NN]
    lane = iota((MCAP, 2 * NN), 1)
    lane = jnp.where(lane >= NN, lane - NN, lane)
    keep = lane < own_ref[:, 0:1]
    parts = []
    for c in range(2):
        part = jnp.concatenate(
            [both[c * 16 : c * 16 + HALF], both[32 + c * 16 : 32 + c * 16 + HALF]], 0
        )
        parts.append(jnp.where(keep, part, 0.0))
    cut = 11 * LANE
    out_ref[:, :cut] = parts[0][:, :cut]
    stores = []

    def store(lanes):
        for r in range(0, MCAP, 8):
            stores.append(
                pltpu.make_async_copy(
                    out_ref.at[pl.ds(r, 8), lanes],
                    out_hbm.at[0, pl.ds(r, 8), lanes],
                    sems.at[len(stores)],
                )
            )
            stores[-1].start()

    store(pl.ds(0, cut))
    out_ref[:, cut:] = jnp.concatenate([parts[0][:, cut:], parts[1]], 1)
    store(pl.ds(cut, 4 * NN - cut))
    for copy in stores:
        copy.wait()


def vmem():
    return pl.BlockSpec(memory_space=pltpu.VMEM)


def hbm():
    return pl.BlockSpec(memory_space=pltpu.HBM)


def held(x):
    return pltpu.with_memory_space_constraint(x, pltpu.VMEM)


def far(x):
    return pltpu.with_memory_space_constraint(x, pltpu.HBM)


def order_levels(level_order, fields):
    args = (level_order.reshape(1, N_GX), fields.transpose(1, 0, 2))
    return pl.pallas_call(
        order_kernel,
        out_shape=pltpu.VMEM((N_GX, 24, LANE), BF16),
        in_specs=[hbm() for _ in args],
        out_specs=vmem(),
        scratch_shapes=[
            pltpu.SMEM((1, N_GX), jnp.int32),
            pltpu.VMEM(args[1].shape, BF16),
            pltpu.SemaphoreType.DMA((1 + -(-ROWS_Y // FETCH_ROWS),)),
        ],
        name="order_levels",
        cost_estimate=pl.CostEstimate(flops=4_000_000_000, bytes_accessed=100_000, transcendentals=0),
        compiler_params=pltpu.CompilerParams(vmem_limit_bytes=VMEM_LIMIT),
    )(*(far(x) for x in args))


def x_transform(grid, m_owner, n_count, cos_x, sin_x):
    args = (grid, m_owner.reshape(1, M), n_count.reshape(1, M), cos_x, sin_x, jnp.asarray(x_flip()))
    return pl.pallas_call(
        x_kernel,
        out_shape=(
            pltpu.VMEM((N_GY * HALF, LANE), BF16),
            pltpu.VMEM((MCAP, LANE), jnp.int32),
        ),
        in_specs=[vmem() for _ in args],
        out_specs=(vmem(), vmem()),
        name="x_transform",
        compiler_params=pltpu.CompilerParams(vmem_limit_bytes=VMEM_LIMIT),
    )(*(held(x) for x in args))


def y_transform(arrived, own, cos_y, sin_y):
    args = (arrived, own, cos_y, sin_y, *(jnp.asarray(t) for t in y_selections()))
    return pl.pallas_call(
        y_kernel,
        out_shape=jax.ShapeDtypeStruct((1, MCAP, 4 * NN), F32),
        in_specs=[vmem() for _ in args],
        out_specs=hbm(),
        scratch_shapes=[
            pltpu.VMEM((N_GY * HALF + 16, LANE), BF16),
            pltpu.VMEM((MCAP, 4 * NN), F32),
            pltpu.SemaphoreType.DMA((6,)),
        ],
        name="y_transform",
        compiler_params=pltpu.CompilerParams(vmem_limit_bytes=VMEM_LIMIT),
    )(*(held(x) for x in args))


def body(fields, level_order, m_owner, n_count):
    cos_x, sin_x = (jnp.asarray(t) for t in x_tables())
    cos_y, sin_y = (jnp.asarray(t) for t in y_tables())
    ordered = order_levels(level_order, fields)
    grid = lax.all_to_all(ordered, "gx", split_axis=0, concat_axis=0, tiled=True)
    outgoing, own = x_transform(grid, m_owner, n_count, cos_x, sin_x)
    outgoing = outgoing.reshape(N_GY * HALF // 4, 4, LANE)
    arrived = lax.all_to_all(outgoing, "gy", split_axis=0, concat_axis=0, tiled=True)
    arrived = arrived.reshape(N_GY * HALF, LANE)
    return y_transform(arrived, own, cos_y, sin_y)


def solution(mesh):
    in_specs = (P(None, "gy", "gx"), P(), P(), P())
    out_specs = P("gx", "gy", None)
    return jax.shard_map(body, mesh=mesh, in_specs=in_specs, out_specs=out_specs, check_vma=False)
```

```python
import math

import jax
import jax.numpy as jnp
import numpy as np
from jax import lax
from jax.experimental import pallas as pl
from jax.experimental.pallas import tpu as pltpu
from jax.sharding import PartitionSpec as P

NX = 2048
NY = 1472
M = 1024
NN = 736
MCAP = 24
HALF = MCAP // 2
N_GY = 64
N_GX = 16
ROWS_Y = 23
FETCH_ROWS = 4
LANE = 128
VMEM_LIMIT = 32 << 20
F32 = jnp.float32
BF16 = jnp.bfloat16


def mode_tables(extent, mode_total):
    middle = extent // 2
    points = np.arange(middle + 1, dtype=np.int64)
    orders = np.arange(mode_total, dtype=np.int64)
    phases = (points[:, None] * orders[None, :] % extent).astype(np.float32) * np.float32(
        2.0 * math.pi / extent
    )
    weight = np.where((points == 0) | (points == middle), 0.5, 1.0).astype(np.float32)
    factor = np.float32(1.0 / math.sqrt(extent))
    cos_even = weight[:, None] * np.cos(phases) * factor
    sin_odd = -np.sin(phases) * factor
    return cos_even, sin_odd


def x_tables():
    cos_x, sin_x = mode_tables(NX, M)
    cos_rows = np.zeros((M + LANE, M), np.float32)
    cos_rows[: M + 1] = cos_x
    return cos_rows.astype(BF16), sin_x[:M].astype(BF16)


def y_tables():
    cos_y, sin_y = mode_tables(NY, NN)
    half = N_GY // 2
    cos_rows = np.zeros((half, 32, 768), np.float32)
    sin_rows = np.zeros((half, 32, 768), np.float32)
    cos_rows[:, :ROWS_Y, :NN] = cos_y[: half * ROWS_Y].reshape(half, ROWS_Y, NN)
    cos_rows[0, ROWS_Y, :NN] = cos_y[half * ROWS_Y]
    sin_rows[:, :ROWS_Y, :NN] = sin_y[: half * ROWS_Y].reshape(half, ROWS_Y, NN)
    return (
        cos_rows.reshape(half * 32, 768).astype(BF16),
        sin_rows.reshape(half * 32, 768).astype(BF16),
    )


def x_flip():
    flip = np.zeros((2 * LANE, LANE), np.float32)
    for i in range(1, LANE):
        flip[LANE - i, i] = 1.0
    flip[LANE, 0] = 1.0
    return flip.astype(BF16)


def y_selections():
    mirror = np.zeros((5 * LANE, 4 * LANE), np.float32)
    middle = np.zeros((LANE, 4 * LANE), np.float32)
    for g in range(4):
        middle[32 * g, LANE * g + ROWS_Y] = 1.0
        for u in range(4):
            for j in range(ROWS_Y):
                n = LANE * g + 32 * u + j
                if j:
                    mirror[LANE * (3 - u) + 32 * g + ROWS_Y - j, n] = 1.0
                else:
                    mirror[LANE * (4 - u) + 32 * g, n] = 1.0
    return mirror.astype(BF16), middle.astype(BF16)


def iota(shape, dim):
    return lax.broadcasted_iota(jnp.int32, shape, dim)


def onehot(mask):
    return jnp.where(mask, 1.0, 0.0).astype(BF16)


def dot(a, b, contract_b=0):
    return lax.dot_general(a, b, (((1,), (contract_b,)), ((), ())), preferred_element_type=F32)


def order_kernel(level_hbm, fields_hbm, out_ref, level_ref, fields_ref, sems):
    fetches = [pltpu.make_async_copy(level_hbm, level_ref, sems.at[0])]
    for i, first in enumerate(range(0, ROWS_Y, FETCH_ROWS)):
        part = pl.ds(first, min(FETCH_ROWS, ROWS_Y - first))
        fetches.append(
            pltpu.make_async_copy(fields_hbm.at[part], fields_ref.at[part], sems.at[i + 1])
        )
    for fetch in fetches:
        fetch.start()
    rows = N_GX * 24
    lane = iota((24, rows), 1)
    y = iota((24, rows), 0)
    lane = jnp.where(y < ROWS_Y, lane - y * N_GX, -1)
    fetches[0].wait()
    pick = [jnp.where(lane == level_ref[0, r], 1.0, 0.0) for r in range(N_GX)]
    pick = jnp.concatenate(pick, 0).astype(BF16)
    for fetch in fetches[1:]:
        fetch.wait()
    data = fields_ref[...].reshape(ROWS_Y * N_GX, LANE)
    data = jnp.concatenate([data, jnp.zeros((N_GX, LANE), BF16)], 0)
    out_ref[...] = dot(pick, data).astype(BF16).reshape(N_GX, 24, LANE)


def find_slots(owner, count, own_ref):
    blocks = M // LANE
    hot = onehot(iota((N_GY, M), 0) == owner)
    stacked = jnp.concatenate([hot[:, b * LANE : (b + 1) * LANE] for b in range(blocks)], 0)
    source = iota((LANE, 2 * LANE), 0)
    target = iota((LANE, 2 * LANE), 1)
    prefix = dot(stacked, onehot((source < target) | (target >= LANE)))
    before = jnp.zeros((N_GY, LANE), F32)
    within = []
    for b in range(blocks):
        part = prefix[b * N_GY : (b + 1) * N_GY]
        rank = part[:, :LANE] + before
        before = before + part[:, LANE:]
        picked = hot[:, b * LANE : (b + 1) * LANE].astype(F32) * rank
        within.append(jnp.sum(picked, axis=0, keepdims=True))
    within = jnp.concatenate(within, 1).astype(jnp.int32)
    low = jnp.where(within < HALF, owner * HALF + within, -1)
    high = jnp.where(within >= HALF, owner * HALF + within - HALF, -1)
    mine = lax.axis_index("gy") * MCAP + iota((MCAP, M), 0) == owner * MCAP + within
    counts = jnp.sum(jnp.where(mine, count.astype(F32), 0.0), axis=1, keepdims=True)
    own_ref[...] = jnp.broadcast_to(counts, (MCAP, LANE)).astype(jnp.int32)
    return low, high


def slot_rows(keys):
    row = iota((256, LANE), 0).astype(F32).astype(BF16)
    row = jnp.concatenate([row] * (M // LANE), 1)
    blocks = []
    for b in range(N_GY * HALF // 256):
        key = keys - 256 * b
        key = jnp.where((key >= 0) & (key < 256), key, -1).astype(F32).astype(BF16)
        blocks.append(jnp.where(row == key, jnp.ones((), BF16), jnp.zeros((), BF16)))
    return jnp.concatenate(blocks, 0)


def x_kernel(grid_ref, owner_ref, count_ref, cos_ref, sin_ref, flip_ref, out_ref, own_ref):
    keys = find_slots(owner_ref[...], count_ref[...], own_ref)
    half = N_GX // 2
    pairs = [
        jnp.concatenate([grid_ref[N_GX - 1 - b], grid_ref[(N_GX - b) % N_GX]], 1)
        for b in range(half)
    ]
    mirror = dot(jnp.concatenate(pairs, 0), flip_ref[...])
    lead = [grid_ref[b].astype(F32) for b in range(half)]
    even = [(lead[b] + mirror[b * 24 : (b + 1) * 24]).astype(BF16) for b in range(half)]
    odd = [(lead[b] - mirror[b * 24 : (b + 1) * 24]).astype(BF16) for b in range(half)]
    middle = grid_ref[half].astype(F32)
    even.append((middle + middle).astype(BF16))
    across = dot(jnp.concatenate(odd, 1), sin_ref[...])
    along = dot(jnp.concatenate(even, 1), cos_ref[...])
    pad = jnp.zeros((8, M), F32)
    spectra = jnp.concatenate([along, pad, across, pad], 0).astype(BF16)
    none = jnp.zeros((64, M), BF16)
    low, high = (slot_rows(k) for k in keys)
    placed = dot(low, jnp.concatenate([spectra, none], 0), 1)
    placed = placed + dot(high, jnp.concatenate([none, spectra], 0), 1)
    out_ref[...] = placed.astype(BF16)


def y_kernel(
    got_ref, own_ref, cos_ref, sin_ref, mirror_ref, middle_ref, out_hbm, wide_ref, out_ref, sems
):
    half = N_GY // 2
    groups = half // 4
    wide_ref[: N_GY * HALF, :] = got_ref[...]
    wide_ref[N_GY * HALF :, :] = jnp.zeros((16, LANE), BF16)
    got = [wide_ref[HALF * s : HALF * s + 16, :] for s in range(N_GY)]
    lead = jnp.concatenate(
        [jnp.concatenate([got[4 * t + u] for u in range(4)], 1) for t in range(groups)], 0
    )
    back = jnp.concatenate(
        [
            jnp.concatenate([got[(60 - 4 * t + v) % N_GY] for v in range(5)], 1)
            for t in range(groups)
        ],
        0,
    )
    lead = jnp.concatenate(
        [
            jnp.concatenate(
                [got[4 * t + u][:, 32 * g : 32 * g + 32] for g in range(4) for u in range(4)], 1
            )
            for t in range(groups)
        ],
        0,
    ).astype(F32)
    mirror = dot(back, mirror_ref[...])
    middle = dot(got[half], middle_ref[...])
    even = lead + mirror
    odd = (lead - mirror).astype(BF16)
    even = jnp.concatenate([even[:16] + 2.0 * middle, even[16:]], 0).astype(BF16)

    def rows_of(v):
        return jnp.concatenate(
            [
                jnp.concatenate(
                    [v[t * 16 : (t + 1) * 16, g * LANE : (g + 1) * LANE] for t in range(groups)], 1
                )
                for g in range(4)
            ],
            0,
        )

    even = rows_of(even)
    odd = rows_of(odd)
    sin_part = dot(odd, sin_ref[...])
    cos_part = dot(even, cos_ref[...])
    both = jnp.concatenate([cos_part[:, :NN], sin_part[:, :NN]], 1)
    lane = iota((MCAP, 2 * NN), 1)
    lane = jnp.where(lane >= NN, lane - NN, lane)
    keep = lane < own_ref[:, 0:1]
    parts = []
    for c in range(2):
        part = jnp.concatenate(
            [both[c * 16 : c * 16 + HALF], both[32 + c * 16 : 32 + c * 16 + HALF]], 0
        )
        parts.append(jnp.where(keep, part, 0.0))
    cut = 11 * LANE
    out_ref[:, :cut] = parts[0][:, :cut]
    stores = []

    def store(lanes):
        for r in range(0, MCAP, 8):
            stores.append(
                pltpu.make_async_copy(
                    out_ref.at[pl.ds(r, 8), lanes],
                    out_hbm.at[0, pl.ds(r, 8), lanes],
                    sems.at[len(stores)],
                )
            )
            stores[-1].start()

    store(pl.ds(0, cut))
    out_ref[:, cut:] = jnp.concatenate([parts[0][:, cut:], parts[1]], 1)
    store(pl.ds(cut, 4 * NN - cut))
    for copy in stores:
        copy.wait()


def vmem():
    return pl.BlockSpec(memory_space=pltpu.VMEM)


def hbm():
    return pl.BlockSpec(memory_space=pltpu.HBM)


def held(x):
    return pltpu.with_memory_space_constraint(x, pltpu.VMEM)


def far(x):
    return pltpu.with_memory_space_constraint(x, pltpu.HBM)


def order_levels(level_order, fields):
    args = (level_order.reshape(1, N_GX), fields.transpose(1, 0, 2))
    return pl.pallas_call(
        order_kernel,
        out_shape=pltpu.VMEM((N_GX, 24, LANE), BF16),
        in_specs=[hbm() for _ in args],
        out_specs=vmem(),
        scratch_shapes=[
            pltpu.SMEM((1, N_GX), jnp.int32),
            pltpu.VMEM(args[1].shape, BF16),
            pltpu.SemaphoreType.DMA((1 + -(-ROWS_Y // FETCH_ROWS),)),
        ],
        name="order_levels",
        cost_estimate=pl.CostEstimate(flops=4_000_000_000, bytes_accessed=100_000, transcendentals=0),
        compiler_params=pltpu.CompilerParams(vmem_limit_bytes=VMEM_LIMIT),
    )(*(far(x) for x in args))


def x_transform(grid, m_owner, n_count, cos_x, sin_x):
    args = (grid, m_owner.reshape(1, M), n_count.reshape(1, M), cos_x, sin_x, jnp.asarray(x_flip()))
    return pl.pallas_call(
        x_kernel,
        out_shape=(
            pltpu.VMEM((N_GY * HALF, LANE), BF16),
            pltpu.VMEM((MCAP, LANE), jnp.int32),
        ),
        in_specs=[vmem() for _ in args],
        out_specs=(vmem(), vmem()),
        name="x_transform",
        compiler_params=pltpu.CompilerParams(vmem_limit_bytes=VMEM_LIMIT),
    )(*(held(x) for x in args))


def y_transform(arrived, own, cos_y, sin_y):
    args = (arrived, own, cos_y, sin_y, *(jnp.asarray(t) for t in y_selections()))
    return pl.pallas_call(
        y_kernel,
        out_shape=jax.ShapeDtypeStruct((1, MCAP, 4 * NN), F32),
        in_specs=[vmem() for _ in args],
        out_specs=hbm(),
        scratch_shapes=[
            pltpu.VMEM((N_GY * HALF + 16, LANE), BF16),
            pltpu.VMEM((MCAP, 4 * NN), F32),
            pltpu.SemaphoreType.DMA((6,)),
        ],
        name="y_transform",
        compiler_params=pltpu.CompilerParams(vmem_limit_bytes=VMEM_LIMIT),
    )(*(held(x) for x in args))


def body(fields, level_order, m_owner, n_count):
    cos_x, sin_x = (jnp.asarray(t) for t in x_tables())
    cos_y, sin_y = (jnp.asarray(t) for t in y_tables())
    ordered = order_levels(level_order, fields)
    grid = lax.all_to_all(ordered, "gx", split_axis=0, concat_axis=0, tiled=True)
    outgoing, own = x_transform(grid, m_owner, n_count, cos_x, sin_x)
    outgoing = outgoing.reshape(N_GY * HALF // 4, 4, LANE)
    arrived = lax.all_to_all(outgoing, "gy", split_axis=0, concat_axis=0, tiled=True)
    arrived = arrived.reshape(N_GY * HALF, LANE)
    return y_transform(arrived, own, cos_y, sin_y)


def solution(mesh):
    in_specs = (P(None, "gy", "gx"), P(), P(), P())
    out_specs = P("gx", "gy", None)
    return jax.shard_map(body, mesh=mesh, in_specs=in_specs, out_specs=out_specs, check_vma=False)
```

```python
import math

import jax
import jax.numpy as jnp
import numpy as np
from jax import lax
from jax.experimental import pallas as pl
from jax.experimental.pallas import tpu as pltpu
from jax.sharding import PartitionSpec as P

NX = 2048
NY = 1472
M = 1024
NN = 736
MCAP = 24
HALF = MCAP // 2
N_GY = 64
N_GX = 16
ROWS_Y = 23
FETCH_ROWS = 4
LANE = 128
VMEM_LIMIT = 32 << 20
F32 = jnp.float32
BF16 = jnp.bfloat16


def mode_tables(extent, mode_total):
    middle = extent // 2
    points = np.arange(middle + 1, dtype=np.int64)
    orders = np.arange(mode_total, dtype=np.int64)
    phases = (points[:, None] * orders[None, :] % extent).astype(np.float32) * np.float32(
        2.0 * math.pi / extent
    )
    weight = np.where((points == 0) | (points == middle), 0.5, 1.0).astype(np.float32)
    factor = np.float32(1.0 / math.sqrt(extent))
    cos_even = weight[:, None] * np.cos(phases) * factor
    sin_odd = -np.sin(phases) * factor
    return cos_even, sin_odd


def x_tables():
    cos_x, sin_x = mode_tables(NX, M)
    cos_rows = np.zeros((M + LANE, M), np.float32)
    cos_rows[: M + 1] = cos_x
    return cos_rows.astype(BF16), sin_x[:M].astype(BF16)


def y_tables():
    cos_y, sin_y = mode_tables(NY, NN)
    half = N_GY // 2
    cos_rows = np.zeros((half, 32, 768), np.float32)
    sin_rows = np.zeros((half, 32, 768), np.float32)
    cos_rows[:, :ROWS_Y, :NN] = cos_y[: half * ROWS_Y].reshape(half, ROWS_Y, NN)
    cos_rows[0, ROWS_Y, :NN] = cos_y[half * ROWS_Y]
    sin_rows[:, :ROWS_Y, :NN] = sin_y[: half * ROWS_Y].reshape(half, ROWS_Y, NN)
    return (
        cos_rows.reshape(half * 32, 768).astype(BF16),
        sin_rows.reshape(half * 32, 768).astype(BF16),
    )


def x_flip():
    flip = np.zeros((2 * LANE, LANE), np.float32)
    for i in range(1, LANE):
        flip[LANE - i, i] = 1.0
    flip[LANE, 0] = 1.0
    return flip.astype(BF16)


def y_selections():
    mirror = np.zeros((6 * LANE, 4 * LANE), np.float32)
    for g in range(4):
        mirror[LANE * 5 + 32 * g, LANE * g + ROWS_Y] = 2.0
        for u in range(4):
            for j in range(ROWS_Y):
                n = LANE * g + 32 * u + j
                if j:
                    mirror[LANE * (3 - u) + 32 * g + ROWS_Y - j, n] = 1.0
                else:
                    mirror[LANE * (4 - u) + 32 * g, n] = 1.0
    return (mirror.astype(BF16),)


def iota(shape, dim):
    return lax.broadcasted_iota(jnp.int32, shape, dim)


def onehot(mask):
    return jnp.where(mask, 1.0, 0.0).astype(BF16)


def dot(a, b, contract_b=0):
    return lax.dot_general(a, b, (((1,), (contract_b,)), ((), ())), preferred_element_type=F32)


def order_kernel(level_hbm, fields_hbm, out_ref, level_ref, fields_ref, sems):
    fetches = [pltpu.make_async_copy(level_hbm, level_ref, sems.at[0])]
    for i, first in enumerate(range(0, ROWS_Y, FETCH_ROWS)):
        part = pl.ds(first, min(FETCH_ROWS, ROWS_Y - first))
        fetches.append(
            pltpu.make_async_copy(fields_hbm.at[part], fields_ref.at[part], sems.at[i + 1])
        )
    for fetch in fetches:
        fetch.start()
    rows = N_GX * 24
    lane = iota((24, rows), 1)
    y = iota((24, rows), 0)
    lane = jnp.where(y < ROWS_Y, lane - y * N_GX, -1)
    fetches[0].wait()
    pick = [jnp.where(lane == level_ref[0, r], 1.0, 0.0) for r in range(N_GX)]
    pick = jnp.concatenate(pick, 0).astype(BF16)
    for fetch in fetches[1:]:
        fetch.wait()
    data = fields_ref[...].reshape(ROWS_Y * N_GX, LANE)
    data = jnp.concatenate([data, jnp.zeros((N_GX, LANE), BF16)], 0)
    out_ref[...] = dot(pick, data).astype(BF16).reshape(N_GX, 24, LANE)


def find_slots(owner, count, own_ref):
    blocks = M // LANE
    hot = onehot(iota((N_GY, M), 0) == owner)
    stacked = jnp.concatenate([hot[:, b * LANE : (b + 1) * LANE] for b in range(blocks)], 0)
    source = iota((LANE, 2 * LANE), 0)
    target = iota((LANE, 2 * LANE), 1)
    prefix = dot(stacked, onehot((source < target) | (target >= LANE)))
    before = jnp.zeros((N_GY, LANE), F32)
    within = []
    for b in range(blocks):
        part = prefix[b * N_GY : (b + 1) * N_GY]
        rank = part[:, :LANE] + before
        before = before + part[:, LANE:]
        picked = hot[:, b * LANE : (b + 1) * LANE].astype(F32) * rank
        within.append(jnp.sum(picked, axis=0, keepdims=True))
    within = jnp.concatenate(within, 1).astype(jnp.int32)
    low = jnp.where(within < HALF, owner * HALF + within, -1)
    high = jnp.where(within >= HALF, owner * HALF + within - HALF, -1)
    mine = lax.axis_index("gy") * MCAP + iota((MCAP, M), 0) == owner * MCAP + within
    counts = jnp.sum(jnp.where(mine, count.astype(F32), 0.0), axis=1, keepdims=True)
    own_ref[...] = jnp.broadcast_to(counts, (MCAP, LANE)).astype(jnp.int32)
    return low, high


def slot_rows(keys):
    row = iota((256, LANE), 0).astype(F32).astype(BF16)
    row = jnp.concatenate([row] * (M // LANE), 1)
    blocks = []
    for b in range(N_GY * HALF // 256):
        key = keys - 256 * b
        key = jnp.where((key >= 0) & (key < 256), key, -1).astype(F32).astype(BF16)
        blocks.append(jnp.where(row == key, jnp.ones((), BF16), jnp.zeros((), BF16)))
    return jnp.concatenate(blocks, 0)


def x_kernel(grid_ref, owner_ref, count_ref, cos_ref, sin_ref, flip_ref, out_ref, own_ref):
    keys = find_slots(owner_ref[...], count_ref[...], own_ref)
    half = N_GX // 2
    pairs = [
        jnp.concatenate([grid_ref[N_GX - 1 - b], grid_ref[(N_GX - b) % N_GX]], 1)
        for b in range(half)
    ]
    mirror = dot(jnp.concatenate(pairs, 0), flip_ref[...])
    lead = [grid_ref[b].astype(F32) for b in range(half)]
    even = [(lead[b] + mirror[b * 24 : (b + 1) * 24]).astype(BF16) for b in range(half)]
    odd = [(lead[b] - mirror[b * 24 : (b + 1) * 24]).astype(BF16) for b in range(half)]
    middle = grid_ref[half].astype(F32)
    even.append((middle + middle).astype(BF16))
    across = dot(jnp.concatenate(odd, 1), sin_ref[...])
    along = dot(jnp.concatenate(even, 1), cos_ref[...])
    pad = jnp.zeros((8, M), F32)
    spectra = jnp.concatenate([along, pad, across, pad], 0).astype(BF16)
    none = jnp.zeros((64, M), BF16)
    low, high = (slot_rows(k) for k in keys)
    placed = dot(low, jnp.concatenate([spectra, none], 0), 1)
    placed = placed + dot(high, jnp.concatenate([none, spectra], 0), 1)
    out_ref[...] = placed.astype(BF16)


def y_kernel(
    got_ref, own_ref, cos_ref, sin_ref, mirror_ref, out_hbm, wide_ref, out_ref, sems
):
    half = N_GY // 2
    groups = half // 4
    wide_ref[: N_GY * HALF, :] = got_ref[...]
    wide_ref[N_GY * HALF :, :] = jnp.zeros((16, LANE), BF16)
    got = [wide_ref[HALF * s : HALF * s + 16, :] for s in range(N_GY)]
    lead = jnp.concatenate(
        [jnp.concatenate([got[4 * t + u] for u in range(4)], 1) for t in range(groups)], 0
    )
    none = jnp.zeros((16, LANE), BF16)
    back = jnp.concatenate(
        [
            jnp.concatenate(
                [got[(60 - 4 * t + v) % N_GY] for v in range(5)] + [none if t else got[half]], 1
            )
            for t in range(groups)
        ],
        0,
    )
    lead = jnp.concatenate(
        [
            jnp.concatenate(
                [got[4 * t + u][:, 32 * g : 32 * g + 32] for g in range(4) for u in range(4)], 1
            )
            for t in range(groups)
        ],
        0,
    ).astype(F32)
    mirror = dot(back, mirror_ref[...])
    even = lead + mirror
    odd = (lead - mirror).astype(BF16)
    even = even.astype(BF16)

    def rows_of(v):
        return jnp.concatenate(
            [
                jnp.concatenate(
                    [v[t * 16 : (t + 1) * 16, g * LANE : (g + 1) * LANE] for t in range(groups)], 1
                )
                for g in range(4)
            ],
            0,
        )

    even = rows_of(even)
    odd = rows_of(odd)
    sin_part = dot(odd, sin_ref[...])
    cos_part = dot(even, cos_ref[...])
    both = jnp.concatenate([cos_part[:, :NN], sin_part[:, :NN]], 1)
    lane = iota((MCAP, 2 * NN), 1)
    lane = jnp.where(lane >= NN, lane - NN, lane)
    keep = lane < own_ref[:, 0:1]
    parts = []
    for c in range(2):
        part = jnp.concatenate(
            [both[c * 16 : c * 16 + HALF], both[32 + c * 16 : 32 + c * 16 + HALF]], 0
        )
        parts.append(jnp.where(keep, part, 0.0))
    cut = 11 * LANE
    out_ref[:, :cut] = parts[0][:, :cut]
    stores = []

    def store(lanes):
        for r in range(0, MCAP, 8):
            stores.append(
                pltpu.make_async_copy(
                    out_ref.at[pl.ds(r, 8), lanes],
                    out_hbm.at[0, pl.ds(r, 8), lanes],
                    sems.at[len(stores)],
                )
            )
            stores[-1].start()

    store(pl.ds(0, cut))
    out_ref[:, cut:] = jnp.concatenate([parts[0][:, cut:], parts[1]], 1)
    store(pl.ds(cut, 4 * NN - cut))
    for copy in stores:
        copy.wait()


def vmem():
    return pl.BlockSpec(memory_space=pltpu.VMEM)


def hbm():
    return pl.BlockSpec(memory_space=pltpu.HBM)


def held(x):
    return pltpu.with_memory_space_constraint(x, pltpu.VMEM)


def far(x):
    return pltpu.with_memory_space_constraint(x, pltpu.HBM)


def order_levels(level_order, fields):
    args = (level_order.reshape(1, N_GX), fields.transpose(1, 0, 2))
    return pl.pallas_call(
        order_kernel,
        out_shape=pltpu.VMEM((N_GX, 24, LANE), BF16),
        in_specs=[hbm() for _ in args],
        out_specs=vmem(),
        scratch_shapes=[
            pltpu.SMEM((1, N_GX), jnp.int32),
            pltpu.VMEM(args[1].shape, BF16),
            pltpu.SemaphoreType.DMA((1 + -(-ROWS_Y // FETCH_ROWS),)),
        ],
        name="order_levels",
        cost_estimate=pl.CostEstimate(flops=4_000_000_000, bytes_accessed=100_000, transcendentals=0),
        compiler_params=pltpu.CompilerParams(vmem_limit_bytes=VMEM_LIMIT),
    )(*(far(x) for x in args))


def x_transform(grid, m_owner, n_count, cos_x, sin_x):
    args = (grid, m_owner.reshape(1, M), n_count.reshape(1, M), cos_x, sin_x, jnp.asarray(x_flip()))
    return pl.pallas_call(
        x_kernel,
        out_shape=(
            pltpu.VMEM((N_GY * HALF, LANE), BF16),
            pltpu.VMEM((MCAP, LANE), jnp.int32),
        ),
        in_specs=[vmem() for _ in args],
        out_specs=(vmem(), vmem()),
        name="x_transform",
        compiler_params=pltpu.CompilerParams(vmem_limit_bytes=VMEM_LIMIT),
    )(*(held(x) for x in args))


def y_transform(arrived, own, cos_y, sin_y):
    args = (arrived, own, cos_y, sin_y, *(jnp.asarray(t) for t in y_selections()))
    return pl.pallas_call(
        y_kernel,
        out_shape=jax.ShapeDtypeStruct((1, MCAP, 4 * NN), F32),
        in_specs=[vmem() for _ in args],
        out_specs=hbm(),
        scratch_shapes=[
            pltpu.VMEM((N_GY * HALF + 16, LANE), BF16),
            pltpu.VMEM((MCAP, 4 * NN), F32),
            pltpu.SemaphoreType.DMA((6,)),
        ],
        name="y_transform",
        compiler_params=pltpu.CompilerParams(vmem_limit_bytes=VMEM_LIMIT),
    )(*(held(x) for x in args))


def body(fields, level_order, m_owner, n_count):
    cos_x, sin_x = (jnp.asarray(t) for t in x_tables())
    cos_y, sin_y = (jnp.asarray(t) for t in y_tables())
    ordered = order_levels(level_order, fields)
    grid = lax.all_to_all(ordered, "gx", split_axis=0, concat_axis=0, tiled=True)
    outgoing, own = x_transform(grid, m_owner, n_count, cos_x, sin_x)
    outgoing = outgoing.reshape(N_GY * HALF // 4, 4, LANE)
    arrived = lax.all_to_all(outgoing, "gy", split_axis=0, concat_axis=0, tiled=True)
    arrived = arrived.reshape(N_GY * HALF, LANE)
    return y_transform(arrived, own, cos_y, sin_y)


def solution(mesh):
    in_specs = (P(None, "gy", "gx"), P(), P(), P())
    out_specs = P("gx", "gy", None)
    return jax.shard_map(body, mesh=mesh, in_specs=in_specs, out_specs=out_specs, check_vma=False)
```
